256 devices in a mesh: zero: 32 (over y, x, core), tp: 8 (over z).
Axes of the slice: x: 4, y: 4, z: 8, core: 2. Of those that a mesh axis runs over, the one named last changes fastest.
Arguments:
- weight_gate: bfloat16 [2560, 9728], P('zero', 'tp'), may hold values from -0.125 to 0.125
- low_gate: bfloat16 [2560, 16], P('zero'), may hold values from -0.125 to 0.125
- high_gate: bfloat16 [16, 9728], P(None, 'tp'), may hold values from -1.5 to 1.5
- weight_up: bfloat16 [2560, 9728], P('zero', 'tp'), may hold values from -0.125 to 0.125
- low_up: bfloat16 [2560, 16], P('zero'), may hold values from -0.125 to 0.125
- high_up: bfloat16 [16, 9728], P(None, 'tp'), may hold values from -1.5 to 1.5
- weight_down: bfloat16 [9728, 2560], P('tp', 'zero'), may hold values from -0.0625 to 0.0625
- low_down: bfloat16 [9728, 16], P('tp'), may hold values from -0.0625 to 0.0625
- high_down: bfloat16 [16, 2560], P(None, 'zero'), may hold values from -1.5 to 1.5
- norm_train: float32 [2560], P(('zero', 'tp')), may hold values from 0.25 to 1.75
- norm_step: float32 [2560], P(('zero', 'tp')), may hold values from -0.3 to 0.3
Outputs:
- ready_gate: bfloat16 [2560, 9728], P(None, 'tp')
- ready_up: bfloat16 [2560, 9728], P(None, 'tp')
- ready_down: bfloat16 [9728, 2560], P('tp')
- serve_norm: bfloat16 [2560], replicated
The draws below stay inside these ranges and needn't reach their ends.
All inputs are finite; a program needn't handle non-finite values.
Results may differ from the reference program's by a relative error of at most 0.001.
Values may be sent and summed in bfloat16 or wider, within the bound.
No kernel may reach another device: no remote copies, remote signals or barrier semaphores. Data moves between devices by JAX's collectives and lax.ppermute only.
A program may use at most 128 MiB of HBM per device.

```python
import jax
import jax.numpy as jnp

D_MODEL = 2560
D_INNER = 9728
RANK = 16


def shard_levels(own_key, dims, shards, low, top_value):
    def one(dim, parts):
        steps = jax.random.uniform(jax.random.fold_in(jax.random.fold_in(own_key, 6), dim), (parts,), jnp.float32, low / len(shards), top_value / len(shards))
        return jnp.repeat(jnp.exp(steps), dims[dim] // parts).reshape((-1,) + (1,) * (len(dims) - dim - 1))

    loudness = one(*shards[0])
    for cut in shards[1:]:
        loudness = loudness * one(*cut)
    return loudness


def gaussian(stream_key, shape, spread, most, shards=(), kind=jnp.bfloat16):
    array = jax.random.normal(stream_key, shape, jnp.float32) * spread
    if len(shards) > 0:
        array = shard_levels(stream_key, shape, shards, -0.22, 0.18) * array
    return jnp.clip(array, min=-most, max=most).astype(kind)


def setup_inputs(seed: int = 0) -> dict:
    key_of = jax.random.split(jax.random.key(seed), 12)
    return {
        "weight_gate": gaussian(key_of[0], (D_MODEL, D_INNER), D_MODEL ** -0.5, 0.125, ((0, 32), (1, 8))),
        "low_gate": gaussian(key_of[1], (D_MODEL, RANK), D_MODEL ** -0.5, 0.125, ((0, 32),)),
        "high_gate": gaussian(key_of[2], (RANK, D_INNER), RANK ** -0.5, 1.5, ((1, 8),)),
        "weight_up": gaussian(key_of[3], (D_MODEL, D_INNER), D_MODEL ** -0.5, 0.125, ((0, 32), (1, 8))),
        "low_up": gaussian(key_of[4], (D_MODEL, RANK), D_MODEL ** -0.5, 0.125, ((0, 32),)),
        "high_up": gaussian(key_of[5], (RANK, D_INNER), RANK ** -0.5, 1.5, ((1, 8),)),
        "weight_down": gaussian(key_of[6], (D_INNER, D_MODEL), D_INNER ** -0.5, 0.0625, ((0, 8), (1, 32))),
        "low_down": gaussian(key_of[7], (D_INNER, RANK), D_INNER ** -0.5, 0.0625, ((0, 8),)),
        "high_down": gaussian(key_of[8], (RANK, D_MODEL), RANK ** -0.5, 1.5, ((1, 32),)),
        "norm_train": jnp.clip(1.0 + 0.15 * jax.random.normal(key_of[9], (D_MODEL,), jnp.float32), 0.25, 1.75),
        "norm_step": jnp.clip(jax.random.uniform(key_of[10], (D_MODEL,), jnp.float32, -0.3, 0.3) * shard_levels(key_of[10], (D_MODEL,), ((0, 256),), -0.4, 0.0), -0.3, 0.3),
    }


mix_rate = 0.5


def reference(weight_gate, low_gate, high_gate, weight_up, low_up, high_up, weight_down, low_down, high_down, norm_train, norm_step):
    latest_gate = weight_gate.astype(jnp.float32) + mix_rate * jnp.dot(low_gate, high_gate, preferred_element_type=jnp.float32)
    latest_up = weight_up.astype(jnp.float32) + mix_rate * jnp.dot(low_up, high_up, preferred_element_type=jnp.float32)
    latest_down = weight_down.astype(jnp.float32) + mix_rate * jnp.dot(low_down, high_down, preferred_element_type=jnp.float32)
    ready_gate = latest_gate.astype(jnp.bfloat16)
    ready_up = latest_up.astype(jnp.bfloat16)
    ready_down = latest_down.astype(jnp.bfloat16)
    serve_norm = (norm_train + norm_step).astype(jnp.bfloat16)
    return ready_gate, ready_up, ready_down, serve_norm
```

```python
import functools

import jax
import jax.numpy as jnp
from jax import lax
from jax.experimental import pallas as pl
from jax.experimental.pallas import tpu as pltpu
from jax.sharding import Mesh
from jax.sharding import PartitionSpec as P

ZERO = ("zero_0", "zero_1", "zero_2")
ZERO_TP = ("zero_0", "zero_1", "zero_2", "tp")
NY, NX, NZ = 4, 4, 8
ROWS = 80
LANES = 128
FULL = 9
WIDE = 2560

mix_rate = 0.5


CHUNKS = (
    [(3, 0), (3, 1)] + [(0, i) for i in range(9)] + [(1, i) for i in range(4)],
    [(1, i) for i in range(4, 9)] + [(2, i) for i in range(9)],
)


def index_of(y, x, c):
    return (y * NX + x) * 2 + c


def ring_pairs(first, step):
    pairs = []
    for y in range(NY):
        for x in range(NX):
            for c in range(2):
                along_x = (c == 0) == first
                to = (y, (x + step) % NX) if along_x else ((y + step) % NY, x)
                pairs.append((index_of(y, x, c), index_of(*to, c)))
    return pairs


SWAP = [(i, i ^ 1) for i in range(2 * NY * NX)]


def send(value, pairs):
    return lax.ppermute(value, ZERO, pairs)


OFFSETS = (0, -2, -1, 1)
CUT = ROWS + 32


def assemble(tiles, nout, has_old, *refs):
    mine, other = refs[0:5], refs[5:10]
    refs = refs[10:]
    if has_old:
        refs = refs[nout:]
    outs = dict(zip(sorted({p for p, _ in tiles if p < 3} | ({0, 1, 2} if (3, 0) in tiles else set())), refs[:nout]))
    refs = refs[nout:]
    norm_ref = None
    if (3, 1) in tiles:
        norm_ref, refs = refs[0], refs[1:]
    held, stage, sems = refs
    y, x, c = (lax.axis_index(a) for a in ZERO)

    def place(core, a, b):
        a, b = lax.rem(a + 8, 4), lax.rem(b + 8, 4)
        return jnp.where(core == 0, index_of(b, a, 0), index_of(a, b, 1))

    moves = []
    for core, group in ((c, mine), (1 - c, other)):
        a = jnp.where(core == 0, x, y)
        b = jnp.where(core == 0, y, x)
        home, back, ahead, far_a, far_b = group
        for ref, off in ((home, 0), (back, -1), (ahead, 1)):
            for k, step in enumerate(OFFSETS):
                moves.append((ref, k * ROWS, place(core, a + step, b + off), 0, ROWS))
        for k, step in enumerate(OFFSETS):
            row = place(core, a + step, b + 2)
            low, high = k * ROWS, (k + 1) * ROWS
            if low < CUT:
                moves.append((far_a, low, row, 0, min(high, CUT) - low))
            if high > CUT:
                start = max(low, CUT)
                moves.append((far_b, start - CUT, row, start - low, high - start))

    def fill(slot, lane):
        for ref, row, place_of, within, count in moves:
            at = pl.multiple_of(place_of * ROWS + within, 16)
            held[slot, pl.ds(at, count), :] = ref[row : row + count, pl.ds(lane, LANES)]

    def turn(slot):
        for g in range(WIDE // 640):
            span = slice(g * 640, (g + 1) * 640)
            stage[slot, :, span] = held[slot, span, :].T

    runs = []
    for k, (p, i) in enumerate(tiles):
        if runs and p < 3 and runs[-1][0] == p and runs[-1][1] + runs[-1][3] == i:
            runs[-1][3] += 1
        else:
            runs.append([p, i, k, 1])

    for p, i, k, count in runs:
        if p < 3:
            out = outs[p]

            def copy_out(n, slot, out=out, i=i):
                return pltpu.make_async_copy(
                    stage.at[slot],
                    out.at[pl.ds(pl.multiple_of((i + n) * LANES, LANES), LANES)],
                    sems.at[slot],
                )

            @pl.loop(0, count)
            def _(n, k=k, copy_out=copy_out):
                slot = lax.rem(n, 2)

                @pl.when(n >= 2)
                def _():
                    copy_out(n - 2, slot).wait()

                fill(slot, pl.multiple_of((k + n) * LANES, LANES))
                turn(slot)
                copy_out(n, slot).start()

            for n in range(max(0, count - 2), count):
                copy_out(n, n % 2).wait()
        else:
            fill(0, k * LANES)
            turn(0)
            half = LANES // 2
            parts = ((0, 0), (1, half)) if i == 0 else ((2, 0),)
            copies = [
                pltpu.make_async_copy(
                    stage.at[0, pl.ds(at, half)],
                    outs[q].at[pl.ds(FULL * LANES, half)],
                    sems.at[j],
                )
                for j, (q, at) in enumerate(parts)
            ]
            for copy in copies:
                copy.start()
            if i == 1:
                for n in range(32):
                    norm_ref[n : n + 1, :] = held[0, n * ROWS : n * ROWS + 16, :].astype(jnp.float32)[0:1]
            for copy in copies:
                copy.wait()


def assembled(tiles, mine, other, old):
    touched = sorted({p for p, _ in tiles if p < 3} | ({0, 1, 2} if (3, 0) in tiles else set()))
    rows = FULL * LANES + LANES // 2
    nout = len(touched)
    has_norm = (3, 1) in tiles
    has_old = old is not None
    vmem = pl.BlockSpec(memory_space=pltpu.VMEM)
    hbm = pl.BlockSpec(memory_space=pltpu.HBM)
    operands = list(mine) + list(other)
    in_specs = [vmem] * len(operands)
    aliases = {}
    if has_old:
        for k, p in enumerate(touched):
            aliases[len(operands)] = k
            operands.append(old[p])
            in_specs.append(hbm)
    out_shape = [jax.ShapeDtypeStruct((rows, WIDE), jnp.bfloat16)] * nout
    out_specs = [hbm] * nout
    if has_norm:
        out_shape.append(jax.ShapeDtypeStruct((32, LANES), jnp.float32))
        out_specs.append(vmem)
    res = pl.pallas_call(
        functools.partial(assemble, tiles, nout, has_old),
        out_shape=out_shape,
        in_specs=in_specs,
        out_specs=out_specs,
        input_output_aliases=aliases,
        scratch_shapes=[
            pltpu.VMEM((2, WIDE, LANES), jnp.bfloat16),
            pltpu.VMEM((2, LANES, WIDE), jnp.bfloat16),
            pltpu.SemaphoreType.DMA((2,)),
        ],
        cost_estimate=pl.CostEstimate(
            flops=int(8e9), bytes_accessed=len(tiles) * LANES * WIDE * 4, transcendentals=0
        ),
        compiler_params=pltpu.CompilerParams(vmem_limit_bytes=20 << 20),
    )(*operands)
    new = dict(old or {})
    for k, p in enumerate(touched):
        new[p] = res[k]
    return new, (res[nout] if has_norm else None)


def local(
    weight_gate,
    low_gate,
    high_gate,
    weight_up,
    low_up,
    high_up,
    weight_down,
    low_down,
    high_down,
    norm_train,
    norm_step,
):
    def merged(weight, low, high):
        latest = weight.astype(jnp.float32) + mix_rate * jnp.dot(
            low, high, preferred_element_type=jnp.float32
        )
        return latest.astype(jnp.bfloat16)

    blocks = [
        merged(weight_gate, low_gate, high_gate),
        merged(weight_up, low_up, high_up),
        merged(weight_down, low_down, high_down).T,
    ]
    gain = (norm_train + norm_step).astype(jnp.bfloat16)
    gain = jnp.pad(gain[None], ((0, ROWS - 1), (0, LANES // 2 - gain.shape[0])))
    cut = FULL * LANES
    spare = [
        jnp.concatenate([blocks[0][:, cut:], blocks[1][:, cut:]], axis=1),
        jnp.concatenate([blocks[2][:, cut:], gain], axis=1),
    ]

    def tile(p, i):
        return spare[i] if p == 3 else blocks[p][:, i * LANES : (i + 1) * LANES]

    outs, norms = None, None
    for tiles in CHUNKS:
        own = jnp.concatenate([tile(p, i) for p, i in tiles], axis=1)
        back = send(own, ring_pairs(True, 1))
        ahead = send(own, ring_pairs(True, -1))
        far = send(back, ring_pairs(True, 1))
        bundle = jnp.concatenate([own, far, back, ahead], axis=0)
        bundle_back = send(bundle, ring_pairs(False, 1))
        bundle_ahead = send(bundle, ring_pairs(False, -1))
        far_a = send(bundle_back[:CUT], ring_pairs(False, 1))
        far_b = send(bundle_ahead[CUT:], ring_pairs(False, -1))
        mine = (bundle, bundle_back, bundle_ahead, far_a, far_b)
        other = tuple(send(m, SWAP) for m in mine)
        outs, got = assembled(tiles, mine, other, outs)
        if got is not None:
            norms = got

    width = norm_train.shape[0]
    table = norms[:, LANES // 2 : LANES // 2 + width].astype(jnp.bfloat16)[None]
    z = lax.axis_index("tp")
    for bit in (1, 2, 4):
        there = lax.ppermute(table, "tp", [(k, k ^ bit) for k in range(NZ)])
        table = jnp.where(
            (z & bit) == 0,
            jnp.concatenate([table, there], axis=0),
            jnp.concatenate([there, table], axis=0),
        )
    serve_norm = table.transpose(1, 0, 2).reshape(-1)
    return (outs[0].T, outs[1].T, outs[2], serve_norm)


def solution(mesh):
    finer = Mesh(
        mesh.devices.reshape(NY, NX, 2, mesh.shape["tp"]), ("zero_0", "zero_1", "zero_2", "tp")
    )
    return jax.shard_map(
        local,
        mesh=finer,
        in_specs=(
            P(ZERO, "tp"),
            P(ZERO, None),
            P(None, "tp"),
            P(ZERO, "tp"),
            P(ZERO, None),
            P(None, "tp"),
            P("tp", ZERO),
            P("tp", None),
            P(None, ZERO),
            P(ZERO_TP),
            P(ZERO_TP),
        ),
        out_specs=(P(None, "tp"), P(None, "tp"), P("tp", None), P()),
        check_vma=False,
    )
```
